128 devices in a mesh: fld: 1, col: 2 (over core), row: 64 (over z, y, x).
Axes of the slice: x: 4, y: 4, z: 4, core: 2. Of those that a mesh axis runs over, the one named last changes fastest.
Arguments:
- u_real: float32 [4, 256, 256, 256], P('fld', None, 'row', 'col')
- u_imag: float32 [4, 256, 256, 256], P('fld', None, 'row', 'col')
- g_filter: float32 [256, 256, 256], P('row', 'col')
Outputs:
- output 1: float32 [4, 256, 256, 256], P('fld', 'row', 'col')
- output 2: float32 [4, 256, 256, 256], P('fld', 'row', 'col')
All inputs are finite; a program needn't handle non-finite values.
Results may differ from the reference program's by a relative error of at most 0.001.
Values are sent between devices in bfloat16 or wider.
A program may use at most 1 GiB of HBM per device.

```python
import jax
import jax.numpy as jnp
from jax import lax

N = 256
BATCH = 4


def setup_inputs(seed: int = 0, part: int = 0) -> dict:
    root_key = jax.random.key(seed)
    field_key = jax.random.fold_in(jax.random.fold_in(root_key, 1), part)
    key_re, key_im = jax.random.split(field_key)
    u_real = jax.random.normal(key_re, (BATCH, N, N, N), jnp.float32)
    u_imag = jax.random.normal(key_im, (BATCH, N, N, N), jnp.float32)
    wave_num = ((jnp.arange(N) + N // 2) % N - N // 2).astype(jnp.float32)
    wave_sq = wave_num * wave_num
    k_sq = wave_sq[:, None, None] + wave_sq[None, :, None] + wave_sq[None, None, :]
    profile = 2.0 / (1.0 + 16.0 * k_sq / (N * N))
    jitter = jax.random.uniform(jax.random.fold_in(root_key, 2), (N, N, N), jnp.float32)
    g_filter = profile * (0.5 + jitter)
    return {"u_real": u_real, "u_imag": u_imag, "g_filter": g_filter}


def reference(u_real, u_imag, g_filter):
    def one_field(field_pair):
        field_re, field_im = field_pair
        spectrum = jnp.fft.fftn(field_re + 1j * field_im, norm="ortho")
        filtered = spectrum * g_filter
        return jnp.real(filtered).astype(jnp.float32), jnp.imag(filtered).astype(jnp.float32)
    w_real, w_imag = lax.map(one_field, (u_real, u_imag))
    return w_real, w_imag
```

```python
import random

import jax
import jax.numpy as jnp
import numpy as np
from jax import lax
from jax.experimental import pallas as pl
from jax.experimental.pallas import tpu as pltpu
from jax.sharding import PartitionSpec as P

MESH = pl.DeviceIdType.MESH
N = 256
FIELDS = 4
HIGHEST = lax.Precision.HIGHEST
F32 = jnp.float32


def dft_blocks():
    steps = np.outer(np.arange(N), np.arange(N)) % N
    angles = steps * (2.0 * np.pi / N)
    cos_part, sin_part = np.cos(angles) / np.sqrt(N), np.sin(angles) / np.sqrt(N)
    real_rows = np.stack([cos_part, sin_part], axis=1)
    imag_rows = np.stack([-sin_part, cos_part], axis=1)
    return np.stack([real_rows, imag_rows])


def matrices():
    full = dft_blocks()
    x_mat = full.reshape(2, 64, 4, 2, N).transpose(1, 0, 2, 3, 4).reshape(512, 512)
    y_mat = full.reshape(2, 2, 128, 2, 64, 4).transpose(1, 0, 2, 3, 5, 4).reshape(512, 512)
    z_mat = full.transpose(2, 3, 0, 1).reshape(512, 512)
    return [m.astype(np.float32) for m in (x_mat, y_mat, z_mat)]


def link_use(offset):
    use = [0] * 6
    for k in range(3):
        if offset[k] in (1, 2):
            use[2 * k] += 1
        if offset[k] in (3, 2):
            use[2 * k + 1] += 1
    return use


def send_order(seed=0):
    rng = random.Random(seed)
    left = [(s % 4, (s // 4) % 4, s // 16) for s in range(1, 64)]
    rng.shuffle(left)
    total, order = [0] * 6, []
    while left:

        def cost(offset):
            after = [a + b for a, b in zip(total, link_use(offset))]
            mean = sum(after) / 6
            return max(after) - min(after), sum((v - mean) ** 2 for v in after), -sum(link_use(offset))

        best = min(left, key=cost)
        left.remove(best)
        order.append(best)
        total = [a + b for a, b in zip(total, link_use(best))]
    return order


ORDER = send_order()


def kernel(ur_hbm, ui_hbm, g_hbm, xm_hbm, ym_hbm, zm_hbm, wr_hbm, wi_hbm,
           u_buf, xm, ym, zm, g_buf, cols, send, recv, planes, ysend, zbuf, wbuf,
           in_sem, send_sem, recv_sem, pair_send, pair_recv, out_sem):
    row, col = lax.axis_index("row"), lax.axis_index("col")
    cz, cy, cx = row // 16, (row // 4) % 4, row % 4
    sign = 1 - 2 * col

    def peer(offset):
        dx, dy, dz = offset
        return ((cz + sign * dz + 4) % 4) * 16 + ((cy + sign * dy + 4) % 4) * 4 + (cx + sign * dx + 4) % 4

    barrier = pltpu.get_barrier_semaphore()
    for offset in ORDER:
        pl.semaphore_signal(barrier, 1, device_id=(0, col, peer(offset)), device_id_type=MESH)
    pl.semaphore_signal(barrier, 1, device_id=(0, 1 - col, row), device_id_type=MESH)

    def load_u(f, part):
        src = (ur_hbm, ui_hbm)[part]
        return pltpu.make_async_copy(src.at[f], u_buf.at[f, part], in_sem.at[2 * f + part])

    x_load = pltpu.make_async_copy(xm_hbm, xm, in_sem.at[8])
    y_load = pltpu.make_async_copy(ym_hbm, ym, in_sem.at[9])
    z_load = pltpu.make_async_copy(zm_hbm, zm, in_sem.at[10])
    g_load = pltpu.make_async_copy(g_hbm, g_buf, in_sem.at[11])
    load_u(0, 0).start()
    load_u(0, 1).start()
    x_load.start()
    for f in range(1, FIELDS):
        load_u(f, 0).start()
        load_u(f, 1).start()
    y_load.start()
    z_load.start()
    g_load.start()
    x_load.wait()

    def x_step(f):
        load_u(f, 0).wait()
        load_u(f, 1).wait()
        for half in range(2):
            for part in range(2):
                for k in range(2):
                    cols[pl.ds(part * 256, 256), pl.ds(k * 128, 128)] = u_buf[f, part, pl.ds(2 * half + k, 256, stride=4), :]
            out = jnp.dot(xm[...], cols[...], precision=HIGHEST, preferred_element_type=F32)
            send[f, 2 * half] = out[:, :128]
            send[f, 2 * half + 1] = out[:, 128:]

    mine = pl.ds(pl.multiple_of(row * 8, 8), 8)

    def send_field(f):
        for offset in ORDER:
            to = peer(offset)
            pltpu.make_async_remote_copy(
                src_ref=send.at[f, :, pl.ds(pl.multiple_of(to * 8, 8), 8), :],
                dst_ref=recv.at[f, :, mine, :],
                send_sem=send_sem.at[f],
                recv_sem=recv_sem.at[f],
                device_id=(0, col, to),
                device_id_type=MESH,
            ).start()
        for yy in range(4):
            recv[f, yy, mine, :] = send[f, yy, mine, :]

    x_step(0)
    pl.semaphore_wait(barrier, len(ORDER) + 1)
    send_field(0)

    @pl.loop(1, FIELDS)
    def _(f):
        x_step(f)
        send_field(f)

    y_load.wait()
    z_load.wait()
    g_load.wait()
    other = 1 - col

    def pair_copy(f, p):
        return pltpu.make_async_remote_copy(
            src_ref=ysend.at[f, p],
            dst_ref=zbuf.at[f, p, col],
            send_sem=pair_send.at[2 * f + p],
            recv_sem=pair_recv.at[2 * f + p],
            device_id=(0, other, row),
            device_id_type=MESH,
        )

    def y_step(f, p):
        for part in range(2):
            for yy in range(4):
                for k in range(2):
                    planes[pl.ds(part * 256 + yy * 64, 64), pl.ds(k * 128, 128)] = recv[f, yy, pl.ds(part * 4 + 2 * p + k, 64, stride=8), :]
        theirs = jnp.dot(ym[pl.ds(pl.multiple_of(other * 256, 256), 256), :], planes[...], precision=HIGHEST, preferred_element_type=F32)
        for part in range(2):
            for k in range(2):
                ysend[f, p, part, pl.ds(k * 128, 128), :] = theirs[part * 128 : part * 128 + 128, k * 128 : k * 128 + 128]
        pair_copy(f, p).start()
        ours = jnp.dot(ym[pl.ds(pl.multiple_of(col * 256, 256), 256), :], planes[...], precision=HIGHEST, preferred_element_type=F32)
        for part in range(2):
            for k in range(2):
                zbuf[f, p, col, part, pl.ds(k * 128, 128), :] = ours[part * 128 : part * 128 + 128, k * 128 : k * 128 + 128]

    def out_copies(f, p):
        return [
            pltpu.make_async_copy(wbuf.at[f, part, pl.ds(2 * p, 2)], (wr_hbm, wi_hbm)[part].at[f, pl.ds(2 * p, 2)], out_sem.at[2 * f + p, part])
            for part in range(2)
        ]

    def z_step(f, p):
        pair_copy(f, p).wait_recv()
        lines = jnp.concatenate([zbuf[f, p, h, part] for part in range(2) for h in range(2)], axis=1)
        out = jnp.dot(lines, zm[...], precision=HIGHEST, preferred_element_type=F32)
        for part in range(2):
            for k in range(2):
                wbuf[f, part, 2 * p + k] = out[k * 128 : k * 128 + 128, part * 256 : part * 256 + 256] * g_buf[2 * p + k]
        for copy in out_copies(f, p):
            copy.start()

    @pl.loop(0, FIELDS)
    def _(f):
        pltpu.make_async_copy(recv.at[f, :, pl.ds(0, 504), :], recv.at[f, :, pl.ds(0, 504), :], recv_sem.at[f]).wait()
        y_step(f, 0)

        @pl.when(f > 0)
        def _():
            z_step(f - 1, 1)

        y_step(f, 1)
        z_step(f, 0)

    z_step(FIELDS - 1, 1)

    @pl.loop(0, FIELDS)
    def _(f):
        pltpu.make_async_copy(send.at[f, :, pl.ds(0, 504), :], send.at[f, :, pl.ds(0, 504), :], send_sem.at[f]).wait()
        for p in range(2):
            pair_copy(f, p).wait_send()
            for copy in out_copies(f, p):
                copy.wait()


def solution(mesh):
    mats = matrices()

    def local_forward(u_real, u_imag, g_filter):
        flat = (FIELDS, 4 * N, 128)
        any_spec = pl.BlockSpec(memory_space=pl.ANY)
        hbm_spec = pl.BlockSpec(memory_space=pltpu.HBM)
        out = jax.ShapeDtypeStruct((FIELDS, 4, 128, N), F32)
        return pl.pallas_call(
            kernel,
            out_shape=(out, out),
            in_specs=[hbm_spec] * 6,
            out_specs=(hbm_spec, hbm_spec),
            scratch_shapes=[
                pltpu.VMEM((FIELDS, 2, 4 * N, 128), F32),
                pltpu.VMEM((512, 512), F32),
                pltpu.VMEM((512, 512), F32),
                pltpu.VMEM((512, 512), F32),
                pltpu.VMEM((4, 128, N), F32),
                pltpu.VMEM((512, 256), F32),
                pltpu.VMEM((FIELDS, 4, 512, 128), F32),
                pltpu.VMEM((FIELDS, 4, 512, 128), F32),
                pltpu.VMEM((512, 256), F32),
                pltpu.VMEM((FIELDS, 2, 2, 256, 128), F32),
                pltpu.VMEM((FIELDS, 2, 2, 2, 256, 128), F32),
                pltpu.VMEM((FIELDS, 2, 4, 128, N), F32),
                pltpu.SemaphoreType.DMA((12,)),
                pltpu.SemaphoreType.DMA((FIELDS,)),
                pltpu.SemaphoreType.DMA((FIELDS,)),
                pltpu.SemaphoreType.DMA((2 * FIELDS,)),
                pltpu.SemaphoreType.DMA((2 * FIELDS,)),
                pltpu.SemaphoreType.DMA((2 * FIELDS, 2)),
            ],
            compiler_params=pltpu.CompilerParams(collective_id=0, has_side_effects=True, vmem_limit_bytes=56 * 2**20),
        )(u_real.reshape(flat), u_imag.reshape(flat), g_filter, *[jnp.asarray(m) for m in mats])

    field_spec = P("fld", None, "row", "col")
    out_spec = P("fld", "row", "col", None)
    return jax.shard_map(local_forward, mesh=mesh, in_specs=(field_spec, field_spec, P("row", "col", None)), out_specs=(out_spec, out_spec), check_vma=False)
```

```python
import jax
import jax.numpy as jnp
import numpy as np
from jax import lax
from jax.experimental import pallas as pl
from jax.experimental.pallas import tpu as pltpu
from jax.sharding import PartitionSpec as P

MESH = pl.DeviceIdType.MESH
N = 256
FIELDS = 4
HIGHEST = lax.Precision.HIGHEST
F32 = jnp.float32


def dft_blocks():
    steps = np.outer(np.arange(N), np.arange(N)) % N
    angles = steps * (2.0 * np.pi / N)
    cos_part, sin_part = np.cos(angles) / np.sqrt(N), np.sin(angles) / np.sqrt(N)
    real_rows = np.stack([cos_part, sin_part], axis=1)
    imag_rows = np.stack([-sin_part, cos_part], axis=1)
    return np.stack([real_rows, imag_rows])


def matrices():
    full = dft_blocks()
    x_mat = full.reshape(2, 64, 4, 2, N).transpose(1, 0, 2, 3, 4).reshape(512, 512)
    y_mat = full.reshape(2, 2, 128, 2, 64, 4).transpose(1, 0, 2, 3, 5, 4).reshape(512, 512)
    z_mat = full.transpose(2, 3, 0, 1).reshape(512, 512)
    return [m.astype(np.float32) for m in (x_mat, y_mat, z_mat)]


STREAMS = ((2, 1, 0), (1, 0, 2), (0, 2, 1))


def kernel(ur_hbm, ui_hbm, g_hbm, xm_hbm, ym_hbm, zm_hbm, wr_hbm, wi_hbm,
           u_buf, xm, ym, zm, g_buf, cols, send, hop1, hop2, recv, planes, ysend, zbuf, wbuf,
           in_sem, send_sem, recv_sem, pair_send, pair_recv, out_sem):
    row, col = lax.axis_index("row"), lax.axis_index("col")
    other = 1 - col
    coord = (row // 16, (row // 4) % 4, row % 4)
    stride = (16, 4, 1)

    def mate(dim, step):
        there = (coord[dim] + step) % 4
        return there, row + (there - coord[dim]) * stride[dim]

    barrier = pltpu.get_barrier_semaphore()
    pl.semaphore_signal(barrier, 1, device_id=(0, other, row), device_id_type=MESH)
    for step in (1, 3, 2):
        for dim in range(3):
            pl.semaphore_signal(barrier, 1, device_id=(0, col, mate(dim, step)[1]), device_id_type=MESH)

    def load_u(f, part):
        src = (ur_hbm, ui_hbm)[part]
        return pltpu.make_async_copy(src.at[f], u_buf.at[f, part], in_sem.at[2 * f + part])

    x_load = pltpu.make_async_copy(xm_hbm, xm, in_sem.at[8])
    y_load = pltpu.make_async_copy(ym_hbm, ym, in_sem.at[9])
    z_load = pltpu.make_async_copy(zm_hbm, zm, in_sem.at[10])
    g_load = pltpu.make_async_copy(g_hbm, g_buf, in_sem.at[11])
    load_u(0, 0).start()
    load_u(0, 1).start()
    x_load.start()
    for f in range(1, FIELDS):
        load_u(f, 0).start()
        load_u(f, 1).start()
    y_load.start()
    z_load.start()
    g_load.start()
    x_load.wait()

    def x_step(f):
        load_u(f, 0).wait()
        load_u(f, 1).wait()

        @pl.loop(0, 2)
        def _(half):
            for part in range(2):
                for k in range(2):
                    cols[pl.ds(part * 256, 256), pl.ds(k * 128, 128)] = u_buf[f, part, pl.ds(2 * half + k, 256, stride=4), :]
            out = jnp.dot(xm[...], cols[...], precision=HIGHEST, preferred_element_type=F32)
            for k in range(2):
                send[f, 2 * half + k] = out[:, k * 128 : k * 128 + 128].reshape(4, 4, 4, 8, 128)

    bufs = (send, hop1, hop2, recv)

    def line(ref, f, yy, dim, at):
        where = [slice(None)] * 3
        where[dim] = at
        return ref.at[(f, yy, *where)]

    def forward(f, phase):
        cur, nxt = bufs[phase], bufs[phase + 1]

        def unit(yy, stream):
            dim = STREAMS[stream][phase]
            for step in (1, 3, 2):
                there, to = mate(dim, step)
                pltpu.make_async_remote_copy(
                    src_ref=line(cur, f, yy, dim, there),
                    dst_ref=line(nxt, f, yy, dim, coord[dim]),
                    send_sem=send_sem.at[phase, f, yy],
                    recv_sem=recv_sem.at[phase, f, yy],
                    device_id=(0, col, to),
                    device_id_type=MESH,
                ).start()
            line(nxt, f, yy, dim, coord[dim])[...] = line(cur, f, yy, dim, coord[dim])[...]

        for yy in range(3):
            unit(yy, yy)
        for stream in range(3):

            @pl.when(f % 3 == stream)
            def _():
                unit(3, stream)

    def arrived(f, phase):
        for yy in range(4):
            three = bufs[phase + 1].at[f, yy, pl.ds(0, 3)]
            pltpu.make_async_copy(three, three, recv_sem.at[phase, f, yy]).wait()

    def pair_copy(f, p):
        return pltpu.make_async_remote_copy(
            src_ref=ysend.at[f, p],
            dst_ref=zbuf.at[f, p, col],
            send_sem=pair_send.at[2 * f + p],
            recv_sem=pair_recv.at[2 * f + p],
            device_id=(0, other, row),
            device_id_type=MESH,
        )

    def y_step(f):
        @pl.loop(0, 2)
        def _(p):
            for yy in range(4):
                rows = recv.at[f, yy].reshape(512, 128)
                for part in range(2):
                    for k in range(2):
                        planes[pl.ds(part * 256 + yy * 64, 64), pl.ds(k * 128, 128)] = rows[pl.ds(part * 4 + 2 * p + k, 64, stride=8), :]
            theirs = jnp.dot(ym[pl.ds(pl.multiple_of(other * 256, 256), 256), :], planes[...], precision=HIGHEST, preferred_element_type=F32)
            for part in range(2):
                for k in range(2):
                    ysend[f, p, part, pl.ds(k * 128, 128), :] = theirs[part * 128 : part * 128 + 128, k * 128 : k * 128 + 128]
            pair_copy(f, p).start()
            ours = jnp.dot(ym[pl.ds(pl.multiple_of(col * 256, 256), 256), :], planes[...], precision=HIGHEST, preferred_element_type=F32)
            for part in range(2):
                for k in range(2):
                    zbuf[f, p, col, part, pl.ds(k * 128, 128), :] = ours[part * 128 : part * 128 + 128, k * 128 : k * 128 + 128]

    def out_copies(f, p):
        return [
            pltpu.make_async_copy(wbuf.at[f, part, pl.ds(2 * p, 2)], (wr_hbm, wi_hbm)[part].at[f, pl.ds(2 * p, 2)], out_sem.at[2 * f + p, part])
            for part in range(2)
        ]

    def z_step(f):
        @pl.loop(0, 2)
        def _(p):
            pair_copy(f, p).wait_recv()
            lines = jnp.concatenate([zbuf[f, p, h, part] for part in range(2) for h in range(2)], axis=1)
            out = jnp.dot(lines, zm[...], precision=HIGHEST, preferred_element_type=F32)
            for part in range(2):
                for k in range(2):
                    wbuf[f, part, 2 * p + k] = out[k * 128 : k * 128 + 128, part * 256 : part * 256 + 256] * g_buf[2 * p + k]
            for copy in out_copies(f, p):
                copy.start()

    @pl.loop(0, FIELDS + 4)
    def _(t):
        @pl.when(t < FIELDS)
        def _():
            x_step(t)

            @pl.when(t == 0)
            def _():
                pl.semaphore_wait(barrier, 10)

            forward(t, 0)

        for phase in (1, 2):

            @pl.when((t >= phase) & (t < FIELDS + phase))
            def _():
                arrived(t - phase, phase - 1)
                forward(t - phase, phase)

        @pl.when(t == 3)
        def _():
            y_load.wait()
            z_load.wait()
            g_load.wait()

        @pl.when(t >= 4)
        def _():
            z_step(t - 4)

        @pl.when((t >= 3) & (t < FIELDS + 3))
        def _():
            arrived(t - 3, 2)
            y_step(t - 3)

    @pl.loop(0, FIELDS)
    def _(f):
        for phase in range(3):
            for yy in range(4):
                three = bufs[phase].at[f, yy, pl.ds(0, 3)]
                pltpu.make_async_copy(three, three, send_sem.at[phase, f, yy]).wait()
        for p in range(2):
            pair_copy(f, p).wait_send()
            for copy in out_copies(f, p):
                copy.wait()


def solution(mesh):
    mats = matrices()

    def local_forward(u_real, u_imag, g_filter):
        flat = (FIELDS, 4 * N, 128)
        hbm_spec = pl.BlockSpec(memory_space=pltpu.HBM)
        out = jax.ShapeDtypeStruct((FIELDS, 4, 128, N), F32)
        return pl.pallas_call(
            kernel,
            out_shape=(out, out),
            in_specs=[hbm_spec] * 6,
            out_specs=(hbm_spec, hbm_spec),
            scratch_shapes=[
                pltpu.VMEM((FIELDS, 2, 4 * N, 128), F32),
                pltpu.VMEM((512, 512), F32),
                pltpu.VMEM((512, 512), F32),
                pltpu.VMEM((512, 512), F32),
                pltpu.VMEM((4, 128, N), F32),
                pltpu.VMEM((512, 256), F32),
                *[pltpu.VMEM((FIELDS, 4, 4, 4, 4, 8, 128), F32)] * 4,
                pltpu.VMEM((512, 256), F32),
                pltpu.VMEM((FIELDS, 2, 2, 256, 128), F32),
                pltpu.VMEM((FIELDS, 2, 2, 2, 256, 128), F32),
                pltpu.VMEM((FIELDS, 2, 4, 128, N), F32),
                pltpu.SemaphoreType.DMA((12,)),
                pltpu.SemaphoreType.DMA((3, FIELDS, 4)),
                pltpu.SemaphoreType.DMA((3, FIELDS, 4)),
                pltpu.SemaphoreType.DMA((2 * FIELDS,)),
                pltpu.SemaphoreType.DMA((2 * FIELDS,)),
                pltpu.SemaphoreType.DMA((2 * FIELDS, 2)),
            ],
            compiler_params=pltpu.CompilerParams(collective_id=0, has_side_effects=True, vmem_limit_bytes=56 * 2**20),
        )(u_real.reshape(flat), u_imag.reshape(flat), g_filter, *[jnp.asarray(m) for m in mats])

    field_spec = P("fld", None, "row", "col")
    out_spec = P("fld", "row", "col", None)
    return jax.shard_map(local_forward, mesh=mesh, in_specs=(field_spec, field_spec, P("row", "col", None)), out_specs=(out_spec, out_spec), check_vma=False)
```

```python
import jax
import jax.numpy as jnp
import numpy as np
from jax import lax
from jax.experimental import pallas as pl
from jax.experimental.pallas import tpu as pltpu
from jax.sharding import PartitionSpec as P

MESH = pl.DeviceIdType.MESH
N = 256
FIELDS = 4
HIGHEST = lax.Precision.HIGHEST
F32 = jnp.float32


def dft_blocks():
    steps = np.outer(np.arange(N), np.arange(N)) % N
    angles = steps * (2.0 * np.pi / N)
    cos_part, sin_part = np.cos(angles) / np.sqrt(N), np.sin(angles) / np.sqrt(N)
    real_rows = np.stack([cos_part, sin_part], axis=1)
    imag_rows = np.stack([-sin_part, cos_part], axis=1)
    return np.stack([real_rows, imag_rows])


def matrices():
    full = dft_blocks()
    x_mat = full.reshape(2, 64, 4, 2, N).transpose(1, 0, 2, 3, 4).reshape(512, 512)
    y_mat = full.reshape(2, 2, 128, 2, 64, 4).transpose(1, 0, 2, 3, 5, 4).reshape(512, 512)
    z_mat = full.transpose(2, 3, 0, 1).reshape(512, 512)
    return [m.astype(np.float32) for m in (x_mat, y_mat, z_mat)]


STREAMS = ((2, 1, 0), (1, 0, 2), (0, 2, 1))


def z_product(zbuf, zm, g_buf, f, p):
    lines = jnp.concatenate([zbuf[f, p, h, part] for part in range(2) for h in range(2)], axis=1)
    out = jnp.dot(lines, zm[...], precision=HIGHEST, preferred_element_type=F32)
    return {
        (part, k): out[k * 128 : k * 128 + 128, part * 256 : part * 256 + 256] * g_buf[2 * p + k]
        for part in range(2)
        for k in range(2)
    }


def last_kernel(zbuf, wbuf, zm, g_buf, wr_hbm, wi_hbm, w_last, out_sem, last_sem):
    outs = (wr_hbm, wi_hbm)
    done = [
        pltpu.make_async_copy(wbuf.at[f, part], outs[part].at[f], out_sem.at[2 * f + part])
        for f in range(FIELDS - 1)
        for part in range(2)
    ]
    for copy in done:
        copy.start()
    last = FIELDS - 1
    for p in range(2):
        for (part, k), value in z_product(zbuf, zm, g_buf, last, p).items():
            w_last[part, 2 * p + k] = value
        for part in range(2):
            copy = pltpu.make_async_copy(w_last.at[part, pl.ds(2 * p, 2)], outs[part].at[last, pl.ds(2 * p, 2)], last_sem.at[2 * p + part])
            copy.start()
            done.append(copy)
    for copy in done:
        copy.wait()


def kernel(ur_hbm, ui_hbm, g_hbm, xm_hbm, ym_hbm, zm_hbm, zbuf, wbuf, zm, g_buf,
           u_buf, xm, ym, cols, send, hop1, hop2, recv, planes, ysend,
           in_sem, send_sem, recv_sem, pair_send, pair_recv):
    row, col = lax.axis_index("row"), lax.axis_index("col")
    other = 1 - col
    coord = (row // 16, (row // 4) % 4, row % 4)
    stride = (16, 4, 1)

    def mate(dim, step):
        there = (coord[dim] + step) % 4
        return there, row + (there - coord[dim]) * stride[dim]

    barrier = pltpu.get_barrier_semaphore()
    pl.semaphore_signal(barrier, 1, device_id=(0, other, row), device_id_type=MESH)
    for step in (1, 3, 2):
        for dim in range(3):
            pl.semaphore_signal(barrier, 1, device_id=(0, col, mate(dim, step)[1]), device_id_type=MESH)

    def load_u(f, part):
        src = (ur_hbm, ui_hbm)[part]
        return pltpu.make_async_copy(src.at[f], u_buf.at[f, part], in_sem.at[2 * f + part])

    x_load = pltpu.make_async_copy(xm_hbm, xm, in_sem.at[8])
    y_load = pltpu.make_async_copy(ym_hbm, ym, in_sem.at[9])
    z_load = pltpu.make_async_copy(zm_hbm, zm, in_sem.at[10])
    g_load = pltpu.make_async_copy(g_hbm, g_buf, in_sem.at[11])
    load_u(0, 0).start()
    load_u(0, 1).start()
    x_load.start()
    for f in range(1, FIELDS):
        load_u(f, 0).start()
        load_u(f, 1).start()
    y_load.start()
    z_load.start()
    g_load.start()
    x_load.wait()

    def x_step(f):
        load_u(f, 0).wait()
        load_u(f, 1).wait()

        @pl.loop(0, 2)
        def _(half):
            for part in range(2):
                for k in range(2):
                    cols[pl.ds(part * 256, 256), pl.ds(k * 128, 128)] = u_buf[f, part, pl.ds(2 * half + k, 256, stride=4), :]
            out = jnp.dot(xm[...], cols[...], precision=HIGHEST, preferred_element_type=F32)
            for k in range(2):
                send[f, 2 * half + k] = out[:, k * 128 : k * 128 + 128].reshape(4, 4, 4, 8, 128)

    bufs = (send, hop1, hop2, recv)

    def line(ref, f, yy, dim, at):
        where = [slice(None)] * 3
        where[dim] = at
        return ref.at[(f, yy, *where)]

    def arrived(f, phase, yy):
        three = bufs[phase + 1].at[f, yy, pl.ds(0, 3)]
        pltpu.make_async_copy(three, three, recv_sem.at[phase, f, yy]).wait()

    def forward(f, phase):
        cur, nxt = bufs[phase], bufs[phase + 1]

        def unit(yy, stream):
            dim = STREAMS[stream][phase]
            if phase:
                arrived(f, phase - 1, yy)
            for step in (1, 3, 2):
                there, to = mate(dim, step)
                pltpu.make_async_remote_copy(
                    src_ref=line(cur, f, yy, dim, there),
                    dst_ref=line(nxt, f, yy, dim, coord[dim]),
                    send_sem=send_sem.at[phase, f, yy],
                    recv_sem=recv_sem.at[phase, f, yy],
                    device_id=(0, col, to),
                    device_id_type=MESH,
                ).start()
            line(nxt, f, yy, dim, coord[dim])[...] = line(cur, f, yy, dim, coord[dim])[...]

        for yy in range(3):
            unit(yy, yy)
        for stream in range(3):

            @pl.when(f % 3 == stream)
            def _():
                unit(3, stream)

    def pair_copy(f, p):
        return pltpu.make_async_remote_copy(
            src_ref=ysend.at[f, p],
            dst_ref=zbuf.at[f, p, col],
            send_sem=pair_send.at[2 * f + p],
            recv_sem=pair_recv.at[2 * f + p],
            device_id=(0, other, row),
            device_id_type=MESH,
        )

    def y_step(f):
        @pl.loop(0, 2)
        def _(p):
            for yy in range(4):
                rows = recv.at[f, yy].reshape(512, 128)
                for part in range(2):
                    for k in range(2):
                        planes[pl.ds(part * 256 + yy * 64, 64), pl.ds(k * 128, 128)] = rows[pl.ds(part * 4 + 2 * p + k, 64, stride=8), :]
            theirs = jnp.dot(ym[pl.ds(pl.multiple_of(other * 256, 256), 256), :], planes[...], precision=HIGHEST, preferred_element_type=F32)
            for part in range(2):
                for k in range(2):
                    ysend[f, p, part, pl.ds(k * 128, 128), :] = theirs[part * 128 : part * 128 + 128, k * 128 : k * 128 + 128]
            ours = jnp.dot(ym[pl.ds(pl.multiple_of(col * 256, 256), 256), :], planes[...], precision=HIGHEST, preferred_element_type=F32)
            for part in range(2):
                for k in range(2):
                    zbuf[f, p, col, part, pl.ds(k * 128, 128), :] = ours[part * 128 : part * 128 + 128, k * 128 : k * 128 + 128]
            pair_copy(f, p).start()

    def z_step(f):
        @pl.loop(0, 2)
        def _(p):
            pair_copy(f, p).wait_recv()
            for (part, k), value in z_product(zbuf, zm, g_buf, f, p).items():
                wbuf[f, part, 2 * p + k] = value

    @pl.loop(0, FIELDS + 4)
    def _(t):
        @pl.when(t < FIELDS)
        def _():
            x_step(t)

            @pl.when(t == 0)
            def _():
                pl.semaphore_wait(barrier, 10)

            forward(t, 0)

        for phase in (1, 2):

            @pl.when((t > phase) & (t <= FIELDS + phase))
            def _():
                forward(t - phase - 1, phase)

        @pl.when(t == 3)
        def _():
            y_load.wait()
            z_load.wait()
            g_load.wait()

        @pl.when(t >= 5)
        def _():
            z_step(t - 5)

        @pl.when((t >= 4) & (t < FIELDS + 4))
        def _():
            for yy in range(4):
                arrived(t - 4, 2, yy)
            y_step(t - 4)

    for p in range(2):
        pair_copy(FIELDS - 1, p).wait_recv()

    @pl.loop(0, FIELDS)
    def _(f):
        for phase in range(3):
            for yy in range(4):
                three = bufs[phase].at[f, yy, pl.ds(0, 3)]
                pltpu.make_async_copy(three, three, send_sem.at[phase, f, yy]).wait()
        for p in range(2):
            pair_copy(f, p).wait_send()


def solution(mesh):
    mats = matrices()

    def local_forward(u_real, u_imag, g_filter):
        flat = (FIELDS, 4 * N, 128)
        hbm_spec = pl.BlockSpec(memory_space=pltpu.HBM)
        vmem_spec = pl.BlockSpec(memory_space=pltpu.VMEM)
        kept = pl.pallas_call(
            kernel,
            out_shape=(
                pltpu.VMEM((FIELDS, 2, 2, 2, 256, 128), F32),
                pltpu.VMEM((FIELDS - 1, 2, 4, 128, N), F32),
                pltpu.VMEM((512, 512), F32),
                pltpu.VMEM((4, 128, N), F32),
            ),
            in_specs=[hbm_spec] * 6,
            out_specs=(vmem_spec,) * 4,
            scratch_shapes=[
                pltpu.VMEM((FIELDS, 2, 4 * N, 128), F32),
                pltpu.VMEM((512, 512), F32),
                pltpu.VMEM((512, 512), F32),
                pltpu.VMEM((512, 256), F32),
                *[pltpu.VMEM((FIELDS, 4, 4, 4, 4, 8, 128), F32)] * 4,
                pltpu.VMEM((512, 256), F32),
                pltpu.VMEM((FIELDS, 2, 2, 256, 128), F32),
                pltpu.SemaphoreType.DMA((12,)),
                pltpu.SemaphoreType.DMA((3, FIELDS, 4)),
                pltpu.SemaphoreType.DMA((3, FIELDS, 4)),
                pltpu.SemaphoreType.DMA((2 * FIELDS,)),
                pltpu.SemaphoreType.DMA((2 * FIELDS,)),
            ],
            compiler_params=pltpu.CompilerParams(collective_id=0, has_side_effects=True, vmem_limit_bytes=55 * 2**20),
        )(u_real.reshape(flat), u_imag.reshape(flat), g_filter, *[jnp.asarray(m) for m in mats])
        out = jax.ShapeDtypeStruct((FIELDS, 4, 128, N), F32)
        return pl.pallas_call(
            last_kernel,
            out_shape=(out, out),
            in_specs=[vmem_spec] * 4,
            out_specs=(hbm_spec, hbm_spec),
            scratch_shapes=[
                pltpu.VMEM((2, 4, 128, N), F32),
                pltpu.SemaphoreType.DMA((2 * FIELDS - 2,)),
                pltpu.SemaphoreType.DMA((4,)),
            ],
            compiler_params=pltpu.CompilerParams(vmem_limit_bytes=40 * 2**20),
        )(*kept)

    field_spec = P("fld", None, "row", "col")
    out_spec = P("fld", "row", "col", None)
    return jax.shard_map(local_forward, mesh=mesh, in_specs=(field_spec, field_spec, P("row", "col", None)), out_specs=(out_spec, out_spec), check_vma=False)
```

```python
import jax
import jax.numpy as jnp
import numpy as np
from jax import lax
from jax.experimental import pallas as pl
from jax.experimental.pallas import tpu as pltpu
from jax.sharding import PartitionSpec as P

MESH = pl.DeviceIdType.MESH
N = 256
FIELDS = 4
HIGHEST = lax.Precision.HIGHEST
F32 = jnp.float32


def dft_blocks():
    steps = np.outer(np.arange(N), np.arange(N)) % N
    angles = steps * (2.0 * np.pi / N)
    cos_part, sin_part = np.cos(angles) / np.sqrt(N), np.sin(angles) / np.sqrt(N)
    real_rows = np.stack([cos_part, sin_part], axis=1)
    imag_rows = np.stack([-sin_part, cos_part], axis=1)
    return np.stack([real_rows, imag_rows])


def matrices():
    full = dft_blocks()
    x_mat = full.reshape(2, 64, 4, 2, N).transpose(1, 0, 2, 3, 4).reshape(512, 512)
    y_mat = full.reshape(2, 2, 128, 2, 64, 4).transpose(1, 0, 2, 3, 5, 4).reshape(512, 512)
    z_mat = full.transpose(2, 3, 0, 1).reshape(512, 512)
    return [m.astype(np.float32) for m in (x_mat, y_mat, z_mat)]


STREAMS = ((2, 1, 0), (1, 0, 2), (0, 2, 1))


def z_product(zbuf, zm, g_buf, f, p):
    lines = jnp.concatenate([zbuf[f, p, h, part] for part in range(2) for h in range(2)], axis=1)
    out = jnp.dot(lines, zm[...], precision=HIGHEST, preferred_element_type=F32)
    return {
        (part, k): out[k * 128 : k * 128 + 128, part * 256 : part * 256 + 256] * g_buf[2 * p + k]
        for part in range(2)
        for k in range(2)
    }


def last_kernel(zbuf, wbuf, zm, g_buf, wr_hbm, wi_hbm, w_last, out_sem, last_sem):
    outs = (wr_hbm, wi_hbm)
    done = [
        pltpu.make_async_copy(wbuf.at[f, part], outs[part].at[f], out_sem.at[2 * f + part])
        for f in range(FIELDS - 1)
        for part in range(2)
    ]
    for copy in done:
        copy.start()
    last = FIELDS - 1
    for p in range(2):
        for (part, k), value in z_product(zbuf, zm, g_buf, last, p).items():
            w_last[part, 2 * p + k] = value
        for part in range(2):
            copy = pltpu.make_async_copy(w_last.at[part, pl.ds(2 * p, 2)], outs[part].at[last, pl.ds(2 * p, 2)], last_sem.at[2 * p + part])
            copy.start()
            done.append(copy)
    for copy in done:
        copy.wait()


def kernel(ur_hbm, ui_hbm, g_hbm, xm_hbm, ym_hbm, zm_hbm, zbuf, wbuf, zm, g_buf,
           u_buf, xm, ym, cols, send, hop1, hop2, recv, planes, ysend,
           in_sem, send_sem, recv_sem, pair_send, pair_recv):
    row, col = lax.axis_index("row"), lax.axis_index("col")
    other = 1 - col
    coord = (row // 16, (row // 4) % 4, row % 4)
    stride = (16, 4, 1)

    def mate(dim, step):
        there = (coord[dim] + step) % 4
        return there, row + (there - coord[dim]) * stride[dim]

    barrier = pltpu.get_barrier_semaphore()
    pl.semaphore_signal(barrier, 1, device_id=(0, other, row), device_id_type=MESH)
    for step in (1, 3, 2):
        for dim in range(3):
            pl.semaphore_signal(barrier, 1, device_id=(0, col, mate(dim, step)[1]), device_id_type=MESH)

    def load_u(f, part):
        src = (ur_hbm, ui_hbm)[part]
        return pltpu.make_async_copy(src.at[f], u_buf.at[f, part], in_sem.at[2 * f + part])

    x_load = pltpu.make_async_copy(xm_hbm, xm, in_sem.at[8])
    y_load = pltpu.make_async_copy(ym_hbm, ym, in_sem.at[9])
    z_load = pltpu.make_async_copy(zm_hbm, zm, in_sem.at[10])
    g_load = pltpu.make_async_copy(g_hbm, g_buf, in_sem.at[11])
    load_u(0, 0).start()
    load_u(0, 1).start()
    x_load.start()
    for f in range(1, FIELDS):
        load_u(f, 0).start()
        load_u(f, 1).start()
    y_load.start()
    z_load.start()
    g_load.start()
    x_load.wait()

    def x_step(f):
        load_u(f, 0).wait()
        load_u(f, 1).wait()

        @pl.loop(0, 2)
        def _(half):
            for part in range(2):
                for k in range(2):
                    cols[pl.ds(part * 256, 256), pl.ds(k * 128, 128)] = u_buf[f, part, pl.ds(2 * half + k, 256, stride=4), :]
            out = jnp.dot(xm[...], cols[...], precision=HIGHEST, preferred_element_type=F32)
            for k in range(2):
                send[f, 2 * half + k] = out[:, k * 128 : k * 128 + 128].reshape(4, 4, 4, 8, 128)

    bufs = (send, hop1, hop2, recv)

    def line(ref, f, yy, dim, at):
        where = [slice(None)] * 3
        where[dim] = at
        return ref.at[(f, yy, *where)]

    def arrived(f, phase, yy):
        three = bufs[phase + 1].at[f, yy, pl.ds(0, 3)]
        pltpu.make_async_copy(three, three, recv_sem.at[phase, f, yy]).wait()

    def forward(f, phase):
        cur, nxt = bufs[phase], bufs[phase + 1]

        def unit(yy, stream):
            dim = STREAMS[stream][phase]
            if phase:
                arrived(f, phase - 1, yy)
            for step in (1, 3, 2):
                there, to = mate(dim, step)
                pltpu.make_async_remote_copy(
                    src_ref=line(cur, f, yy, dim, there),
                    dst_ref=line(nxt, f, yy, dim, coord[dim]),
                    send_sem=send_sem.at[phase, f, yy],
                    recv_sem=recv_sem.at[phase, f, yy],
                    device_id=(0, col, to),
                    device_id_type=MESH,
                ).start()
            line(nxt, f, yy, dim, coord[dim])[...] = line(cur, f, yy, dim, coord[dim])[...]

        for yy in range(3):
            unit(yy, yy)
        for stream in range(3):

            @pl.when(f % 3 == stream)
            def _():
                unit(3, stream)

    def pair_copy(f, p):
        return pltpu.make_async_remote_copy(
            src_ref=ysend.at[f, p],
            dst_ref=zbuf.at[f, p, col],
            send_sem=pair_send.at[2 * f + p],
            recv_sem=pair_recv.at[2 * f + p],
            device_id=(0, other, row),
            device_id_type=MESH,
        )

    def y_step(f):
        @pl.loop(0, 2)
        def _(p):
            for yy in range(4):
                rows = recv.at[f, yy].reshape(512, 128)
                for part in range(2):
                    for k in range(2):
                        planes[pl.ds(part * 256 + yy * 64, 64), pl.ds(k * 128, 128)] = rows[pl.ds(part * 4 + 2 * p + k, 64, stride=8), :]
            theirs = jnp.dot(ym[pl.ds(pl.multiple_of(other * 256, 256), 256), :], planes[...], precision=HIGHEST, preferred_element_type=F32)
            for part in range(2):
                for k in range(2):
                    ysend[f, p, part, pl.ds(k * 128, 128), :] = theirs[part * 128 : part * 128 + 128, k * 128 : k * 128 + 128]
            ours = jnp.dot(ym[pl.ds(pl.multiple_of(col * 256, 256), 256), :], planes[...], precision=HIGHEST, preferred_element_type=F32)
            for part in range(2):
                for k in range(2):
                    zbuf[f, p, col, part, pl.ds(k * 128, 128), :] = ours[part * 128 : part * 128 + 128, k * 128 : k * 128 + 128]
            pair_copy(f, p).start()

    def z_step(f):
        @pl.loop(0, 2)
        def _(p):
            pair_copy(f, p).wait_recv()
            for (part, k), value in z_product(zbuf, zm, g_buf, f, p).items():
                wbuf[f, part, 2 * p + k] = value

    @pl.loop(0, FIELDS + 6)
    def _(t):
        @pl.when(t < FIELDS)
        def _():
            x_step(t)

            @pl.when(t == 0)
            def _():
                pl.semaphore_wait(barrier, 10)

            forward(t, 0)

        for phase in (1, 2):

            @pl.when((t >= 2 * phase) & (t < FIELDS + 2 * phase))
            def _():
                forward(t - 2 * phase, phase)

        @pl.when(t == 6)
        def _():
            y_load.wait()
            z_load.wait()
            g_load.wait()

        @pl.when((t == 7) | (t == 8))
        def _():
            z_step(t - 7)

        @pl.when(t >= 6)
        def _():
            for yy in range(4):
                arrived(t - 6, 2, yy)
            y_step(t - 6)

    z_step(FIELDS - 2)
    for p in range(2):
        pair_copy(FIELDS - 1, p).wait_recv()

    @pl.loop(0, FIELDS)
    def _(f):
        for phase in range(3):
            for yy in range(4):
                three = bufs[phase].at[f, yy, pl.ds(0, 3)]
                pltpu.make_async_copy(three, three, send_sem.at[phase, f, yy]).wait()
        for p in range(2):
            pair_copy(f, p).wait_send()


def solution(mesh):
    mats = matrices()

    def local_forward(u_real, u_imag, g_filter):
        flat = (FIELDS, 4 * N, 128)
        hbm_spec = pl.BlockSpec(memory_space=pltpu.HBM)
        vmem_spec = pl.BlockSpec(memory_space=pltpu.VMEM)
        kept = pl.pallas_call(
            kernel,
            out_shape=(
                pltpu.VMEM((FIELDS, 2, 2, 2, 256, 128), F32),
                pltpu.VMEM((FIELDS - 1, 2, 4, 128, N), F32),
                pltpu.VMEM((512, 512), F32),
                pltpu.VMEM((4, 128, N), F32),
            ),
            in_specs=[hbm_spec] * 6,
            out_specs=(vmem_spec,) * 4,
            scratch_shapes=[
                pltpu.VMEM((FIELDS, 2, 4 * N, 128), F32),
                pltpu.VMEM((512, 512), F32),
                pltpu.VMEM((512, 512), F32),
                pltpu.VMEM((512, 256), F32),
                *[pltpu.VMEM((FIELDS, 4, 4, 4, 4, 8, 128), F32)] * 4,
                pltpu.VMEM((512, 256), F32),
                pltpu.VMEM((FIELDS, 2, 2, 256, 128), F32),
                pltpu.SemaphoreType.DMA((12,)),
                pltpu.SemaphoreType.DMA((3, FIELDS, 4)),
                pltpu.SemaphoreType.DMA((3, FIELDS, 4)),
                pltpu.SemaphoreType.DMA((2 * FIELDS,)),
                pltpu.SemaphoreType.DMA((2 * FIELDS,)),
            ],
            compiler_params=pltpu.CompilerParams(collective_id=0, has_side_effects=True, vmem_limit_bytes=55 * 2**20),
        )(u_real.reshape(flat), u_imag.reshape(flat), g_filter, *[jnp.asarray(m) for m in mats])
        out = jax.ShapeDtypeStruct((FIELDS, 4, 128, N), F32)
        return pl.pallas_call(
            last_kernel,
            out_shape=(out, out),
            in_specs=[vmem_spec] * 4,
            out_specs=(hbm_spec, hbm_spec),
            scratch_shapes=[
                pltpu.VMEM((2, 4, 128, N), F32),
                pltpu.SemaphoreType.DMA((2 * FIELDS - 2,)),
                pltpu.SemaphoreType.DMA((4,)),
            ],
            compiler_params=pltpu.CompilerParams(vmem_limit_bytes=40 * 2**20),
        )(*kept)

    field_spec = P("fld", None, "row", "col")
    out_spec = P("fld", "row", "col", None)
    return jax.shard_map(local_forward, mesh=mesh, in_specs=(field_spec, field_spec, P("row", "col", None)), out_specs=(out_spec, out_spec), check_vma=False)
```

```python
import jax
import jax.numpy as jnp
import numpy as np
from jax import lax
from jax.experimental import pallas as pl
from jax.experimental.pallas import tpu as pltpu
from jax.sharding import PartitionSpec as P

MESH = pl.DeviceIdType.MESH
N = 256
FIELDS = 4
SCALE = 1.0 / 16.0
HIGHEST = lax.Precision.HIGHEST
F32 = jnp.float32


def dft_blocks(length):
    steps = np.outer(np.arange(length), np.arange(length)) % length
    angles = steps * (2.0 * np.pi / length)
    cos_part, sin_part = np.cos(angles), np.sin(angles)
    real_rows = np.stack([cos_part, sin_part], axis=1)
    imag_rows = np.stack([-sin_part, cos_part], axis=1)
    return np.stack([real_rows, imag_rows])


def matrices():
    half, full = dft_blocks(N // 2), dft_blocks(N) * SCALE
    x_mat = half.reshape(2, 64, 2, 2, 128).transpose(1, 0, 2, 3, 4).reshape(256, 256)
    y_mat = half.reshape(2, 2, 64, 2, 32, 4).transpose(1, 0, 2, 3, 5, 4).reshape(256, 256)
    z_mat = full.transpose(2, 3, 0, 1).reshape(512, 512)
    turns = np.arange(N // 2) * (2.0 * np.pi / N)
    y_turns = turns.reshape(32, 4).T.reshape(-1)
    factors = np.stack([np.cos(turns), np.sin(turns), np.cos(y_turns), np.sin(y_turns)])
    factors = np.repeat(factors[:, :, None], 128, axis=2)
    return [m.astype(np.float32) for m in (x_mat, y_mat, z_mat, factors)]


def even_odd(low, high, cos, sin):
    low, high = [v * SCALE for v in low], [v * SCALE for v in high]
    even = [a + b for a, b in zip(low, high)]
    re, im = [a - b for a, b in zip(low, high)]
    return even, [re * cos + im * sin, im * cos - re * sin]


STREAMS = ((2, 1, 0), (1, 0, 2), (0, 2, 1))


def z_product(zbuf, zm, g_buf, f, p):
    lines = jnp.concatenate([zbuf[f, p, h, part] for part in range(2) for h in range(2)], axis=1)
    out = jnp.dot(lines, zm[...], precision=HIGHEST, preferred_element_type=F32)
    return {
        (part, k): out[k * 128 : k * 128 + 128, part * 256 : part * 256 + 256] * g_buf[2 * p + k]
        for part in range(2)
        for k in range(2)
    }


def last_kernel(zbuf, wbuf, zm, g_buf, wr_hbm, wi_hbm, w_last, out_sem, last_sem):
    outs = (wr_hbm, wi_hbm)
    done = [
        pltpu.make_async_copy(wbuf.at[f, part], outs[part].at[f], out_sem.at[2 * f + part])
        for f in range(FIELDS - 1)
        for part in range(2)
    ]
    for copy in done:
        copy.start()
    last = FIELDS - 1
    for p in range(2):
        for (part, k), value in z_product(zbuf, zm, g_buf, last, p).items():
            w_last[part, 2 * p + k] = value
        for part in range(2):
            copy = pltpu.make_async_copy(w_last.at[part, pl.ds(2 * p, 2)], outs[part].at[last, pl.ds(2 * p, 2)], last_sem.at[2 * p + part])
            copy.start()
            done.append(copy)
    for copy in done:
        copy.wait()


def kernel(ur_hbm, ui_hbm, g_hbm, xm_hbm, ym_hbm, zm_hbm, factor_hbm, zbuf, wbuf, zm, g_buf,
           u_buf, xm, ym, factor, cols, send, hop1, hop2, recv, planes, ysend,
           in_sem, send_sem, recv_sem, pair_send, pair_recv):
    row, col = lax.axis_index("row"), lax.axis_index("col")
    other = 1 - col
    coord = (row // 16, (row // 4) % 4, row % 4)
    stride = (16, 4, 1)

    def mate(dim, step):
        there = (coord[dim] + step) % 4
        return there, row + (there - coord[dim]) * stride[dim]

    barrier = pltpu.get_barrier_semaphore()
    pl.semaphore_signal(barrier, 1, device_id=(0, other, row), device_id_type=MESH)
    for step in (1, 3, 2):
        for dim in range(3):
            pl.semaphore_signal(barrier, 1, device_id=(0, col, mate(dim, step)[1]), device_id_type=MESH)

    def load_u(f, part):
        src = (ur_hbm, ui_hbm)[part]
        return pltpu.make_async_copy(src.at[f], u_buf.at[f, part], in_sem.at[2 * f + part])

    x_load = pltpu.make_async_copy(xm_hbm, xm, in_sem.at[8])
    factor_load = pltpu.make_async_copy(factor_hbm, factor, in_sem.at[13])
    y_loads = [
        pltpu.make_async_copy(ym_hbm.at[pl.ds(pl.multiple_of(h * 128, 128), 128), :], ym.at[pl.ds(128 * place, 128), :], in_sem.at[sem])
        for place, h, sem in ((0, other, 9), (1, col, 12))
    ]
    z_load = pltpu.make_async_copy(zm_hbm, zm, in_sem.at[10])
    g_load = pltpu.make_async_copy(g_hbm, g_buf, in_sem.at[11])
    load_u(0, 0).start()
    load_u(0, 1).start()
    x_load.start()
    factor_load.start()
    for f in range(1, FIELDS):
        load_u(f, 0).start()
        load_u(f, 1).start()
    for load in y_loads:
        load.start()
    z_load.start()
    g_load.start()
    x_load.wait()
    factor_load.wait()

    def x_step(f):
        load_u(f, 0).wait()
        load_u(f, 1).wait()

        @pl.loop(0, 2)
        def _(half):
            for k in range(2):
                low, high = [
                    [u_buf[f, part, pl.ds(first + 2 * half + k, 128, stride=4), :] for part in range(2)]
                    for first in (0, 512)
                ]
                for parity, pair in enumerate(even_odd(low, high, factor[0], factor[1])):
                    for part in range(2):
                        cols[pl.ds(part * 128, 128), pl.ds((2 * k + parity) * 128, 128)] = pair[part]
            out = jnp.dot(xm[...], cols[...], precision=HIGHEST, preferred_element_type=F32)
            for k in range(2):
                rows = send.at[f, 2 * half + k].reshape(512, 128)
                for parity in range(2):
                    rows[pl.ds(parity, 256, stride=2), :] = out[:, (2 * k + parity) * 128 : (2 * k + parity) * 128 + 128]

    bufs = (send, hop1, hop2, recv)

    def line(ref, f, yy, dim, at):
        where = [slice(None)] * 3
        where[dim] = at
        return ref.at[(f, yy, *where)]

    def arrived(f, phase, yy):
        three = bufs[phase + 1].at[f, yy, pl.ds(0, 3)]
        pltpu.make_async_copy(three, three, recv_sem.at[phase, f, yy]).wait()

    def forward(f, phase):
        cur, nxt = bufs[phase], bufs[phase + 1]

        def unit(yy, stream):
            dim = STREAMS[stream][phase]
            if phase:
                arrived(f, phase - 1, yy)
            for step in (1, 3, 2):
                there, to = mate(dim, step)
                pltpu.make_async_remote_copy(
                    src_ref=line(cur, f, yy, dim, there),
                    dst_ref=line(nxt, f, yy, dim, coord[dim]),
                    send_sem=send_sem.at[phase, f, yy],
                    recv_sem=recv_sem.at[phase, f, yy],
                    device_id=(0, col, to),
                    device_id_type=MESH,
                ).start()
            line(nxt, f, yy, dim, coord[dim])[...] = line(cur, f, yy, dim, coord[dim])[...]

        for yy in range(3):
            unit(yy, yy)
        for stream in range(3):

            @pl.when(f % 3 == stream)
            def _():
                unit(3, stream)

    def pair_copy(f, p):
        return pltpu.make_async_remote_copy(
            src_ref=ysend.at[f, p],
            dst_ref=zbuf.at[f, p, col],
            send_sem=pair_send.at[2 * f + p],
            recv_sem=pair_recv.at[2 * f + p],
            device_id=(0, other, row),
            device_id_type=MESH,
        )

    def y_step(f):
        @pl.loop(0, 2)
        def _(p):
            for yy in range(4):
                rows = recv.at[f, yy].reshape(512, 128)
                turn = pl.ds(yy * 32, 32)
                for k in range(2):
                    low, high = [
                        [rows[pl.ds(first + part * 4 + 2 * p + k, 32, stride=8), :] for part in range(2)]
                        for first in (0, 256)
                    ]
                    for parity, pair in enumerate(even_odd(low, high, factor[2, turn, :], factor[3, turn, :])):
                        for part in range(2):
                            planes[pl.ds(part * 128 + yy * 32, 32), pl.ds((2 * k + parity) * 128, 128)] = pair[part]
            out = jnp.dot(ym[...], planes[...], precision=HIGHEST, preferred_element_type=F32)
            for part in range(2):
                for k in range(2):
                    for parity in range(2):
                        lanes = slice((2 * k + parity) * 128, (2 * k + parity) * 128 + 128)
                        where = pl.ds(k * 128 + parity, 64, stride=2)
                        ysend[f, p, part, where, :] = out[part * 64 : part * 64 + 64, lanes]
                        zbuf[f, p, col, part, where, :] = out[128 + part * 64 : 128 + part * 64 + 64, lanes]
            pair_copy(f, p).start()

    def z_step(f):
        @pl.loop(0, 2)
        def _(p):
            pair_copy(f, p).wait_recv()
            for (part, k), value in z_product(zbuf, zm, g_buf, f, p).items():
                wbuf[f, part, 2 * p + k] = value

    @pl.loop(0, FIELDS + 6)
    def _(t):
        @pl.when(t < FIELDS)
        def _():
            x_step(t)

            @pl.when(t == 0)
            def _():
                pl.semaphore_wait(barrier, 10)

            forward(t, 0)

        for phase in (1, 2):

            @pl.when((t >= 2 * phase) & (t < FIELDS + 2 * phase))
            def _():
                forward(t - 2 * phase, phase)

        @pl.when(t == 6)
        def _():
            for load in y_loads:
                load.wait()
            z_load.wait()
            g_load.wait()

        @pl.when((t == 7) | (t == 8))
        def _():
            z_step(t - 7)

        @pl.when(t >= 6)
        def _():
            for yy in range(4):
                arrived(t - 6, 2, yy)
            y_step(t - 6)

    z_step(FIELDS - 2)
    for p in range(2):
        pair_copy(FIELDS - 1, p).wait_recv()

    @pl.loop(0, FIELDS)
    def _(f):
        for phase in range(3):
            for yy in range(4):
                three = bufs[phase].at[f, yy, pl.ds(0, 3)]
                pltpu.make_async_copy(three, three, send_sem.at[phase, f, yy]).wait()
        for p in range(2):
            pair_copy(f, p).wait_send()


def solution(mesh):
    mats = matrices()

    def local_forward(u_real, u_imag, g_filter):
        flat = (FIELDS, 4 * N, 128)
        hbm_spec = pl.BlockSpec(memory_space=pltpu.HBM)
        vmem_spec = pl.BlockSpec(memory_space=pltpu.VMEM)
        kept = pl.pallas_call(
            kernel,
            out_shape=(
                pltpu.VMEM((FIELDS, 2, 2, 2, 256, 128), F32),
                pltpu.VMEM((FIELDS - 1, 2, 4, 128, N), F32),
                pltpu.VMEM((512, 512), F32),
                pltpu.VMEM((4, 128, N), F32),
            ),
            in_specs=[hbm_spec] * 7,
            out_specs=(vmem_spec,) * 4,
            scratch_shapes=[
                pltpu.VMEM((FIELDS, 2, 4 * N, 128), F32),
                pltpu.VMEM((256, 256), F32),
                pltpu.VMEM((256, 256), F32),
                pltpu.VMEM((4, 128, 128), F32),
                pltpu.VMEM((256, 512), F32),
                *[pltpu.VMEM((FIELDS, 4, 4, 4, 4, 8, 128), F32)] * 4,
                pltpu.VMEM((256, 512), F32),
                pltpu.VMEM((FIELDS, 2, 2, 256, 128), F32),
                pltpu.SemaphoreType.DMA((14,)),
                pltpu.SemaphoreType.DMA((3, FIELDS, 4)),
                pltpu.SemaphoreType.DMA((3, FIELDS, 4)),
                pltpu.SemaphoreType.DMA((2 * FIELDS,)),
                pltpu.SemaphoreType.DMA((2 * FIELDS,)),
            ],
            compiler_params=pltpu.CompilerParams(collective_id=0, has_side_effects=True, vmem_limit_bytes=55 * 2**20),
        )(u_real.reshape(flat), u_imag.reshape(flat), g_filter, *[jnp.asarray(m) for m in mats])
        out = jax.ShapeDtypeStruct((FIELDS, 4, 128, N), F32)
        return pl.pallas_call(
            last_kernel,
            out_shape=(out, out),
            in_specs=[vmem_spec] * 4,
            out_specs=(hbm_spec, hbm_spec),
            scratch_shapes=[
                pltpu.VMEM((2, 4, 128, N), F32),
                pltpu.SemaphoreType.DMA((2 * FIELDS - 2,)),
                pltpu.SemaphoreType.DMA((4,)),
            ],
            compiler_params=pltpu.CompilerParams(vmem_limit_bytes=40 * 2**20),
        )(*kept)

    field_spec = P("fld", None, "row", "col")
    out_spec = P("fld", "row", "col", None)
    return jax.shard_map(local_forward, mesh=mesh, in_specs=(field_spec, field_spec, P("row", "col", None)), out_specs=(out_spec, out_spec), check_vma=False)
```

```python
import jax
import jax.numpy as jnp
import numpy as np
from jax import lax
from jax.experimental import pallas as pl
from jax.experimental.pallas import tpu as pltpu
from jax.sharding import PartitionSpec as P

MESH = pl.DeviceIdType.MESH
N = 256
FIELDS = 4
SCALE = 1.0 / 16.0
HIGHEST = lax.Precision.HIGHEST
F32 = jnp.float32


def dft_blocks(length):
    steps = np.outer(np.arange(length), np.arange(length)) % length
    angles = steps * (2.0 * np.pi / length)
    cos_part, sin_part = np.cos(angles), np.sin(angles)
    real_rows = np.stack([cos_part, sin_part], axis=1)
    imag_rows = np.stack([-sin_part, cos_part], axis=1)
    return np.stack([real_rows, imag_rows])


def matrices():
    half, full = dft_blocks(N // 2), dft_blocks(N) * SCALE
    x_mat = half.reshape(2, 64, 2, 2, 128).transpose(1, 0, 2, 3, 4).reshape(256, 256)
    y_mat = half.reshape(2, 2, 64, 2, 32, 4).transpose(1, 0, 2, 3, 5, 4).reshape(256, 256)
    z_mat = full.transpose(2, 3, 0, 1).reshape(512, 512)
    turns = np.arange(N // 2) * (2.0 * np.pi / N)
    y_turns = turns.reshape(32, 4).T.reshape(-1)
    factors = np.stack([np.cos(turns), np.sin(turns), np.cos(y_turns), np.sin(y_turns)])
    factors = np.repeat(factors[:, :, None], 128, axis=2)
    return [m.astype(np.float32) for m in (x_mat, y_mat, z_mat, factors)]


def even_odd(low, high, cos, sin):
    low, high = [v * SCALE for v in low], [v * SCALE for v in high]
    even = [a + b for a, b in zip(low, high)]
    re, im = [a - b for a, b in zip(low, high)]
    return even, [re * cos + im * sin, im * cos - re * sin]


STREAMS = ((2, 1, 0), (1, 0, 2), (0, 2, 1))


def z_product(zbuf, zm, g_buf, f, p):
    lines = jnp.concatenate([zbuf[f, p, h, part] for part in range(2) for h in range(2)], axis=1)
    out = jnp.dot(lines, zm[...], precision=HIGHEST, preferred_element_type=F32)
    return {
        (part, k): out[k * 128 : k * 128 + 128, part * 256 : part * 256 + 256] * g_buf[2 * p + k]
        for part in range(2)
        for k in range(2)
    }


def last_kernel(zbuf, wbuf, zm, g_buf, wr_hbm, wi_hbm, w_last, out_sem, last_sem):
    outs = (wr_hbm, wi_hbm)
    done = [
        pltpu.make_async_copy(wbuf.at[f, part], outs[part].at[f], out_sem.at[2 * f + part])
        for f in range(FIELDS - 1)
        for part in range(2)
    ]
    for copy in done:
        copy.start()
    last = FIELDS - 1
    for p in range(2):
        for (part, k), value in z_product(zbuf, zm, g_buf, last, p).items():
            w_last[part, 2 * p + k] = value
        for part in range(2):
            copy = pltpu.make_async_copy(w_last.at[part, pl.ds(2 * p, 2)], outs[part].at[last, pl.ds(2 * p, 2)], last_sem.at[2 * p + part])
            copy.start()
            done.append(copy)
    for copy in done:
        copy.wait()


def kernel(ur_hbm, ui_hbm, g_hbm, xm_hbm, ym_hbm, zm_hbm, factor_hbm, zbuf, wbuf, zm, g_buf,
           u_buf, xm, ym, factor, cols, send, hop1, hop2, recv, planes, ysend,
           in_sem, send_sem, recv_sem, pair_send, pair_recv):
    row, col = lax.axis_index("row"), lax.axis_index("col")
    other = 1 - col
    coord = (row // 16, (row // 4) % 4, row % 4)
    stride = (16, 4, 1)

    def mate(dim, step):
        there = (coord[dim] + step) % 4
        return there, row + (there - coord[dim]) * stride[dim]

    barrier = pltpu.get_barrier_semaphore()
    pl.semaphore_signal(barrier, 1, device_id=(0, other, row), device_id_type=MESH)
    for step in (1, 3, 2):
        for dim in range(3):
            pl.semaphore_signal(barrier, 1, device_id=(0, col, mate(dim, step)[1]), device_id_type=MESH)

    def load_u(f, part):
        src = (ur_hbm, ui_hbm)[part]
        return pltpu.make_async_copy(src.at[f], u_buf.at[f, part], in_sem.at[2 * f + part])

    x_load = pltpu.make_async_copy(xm_hbm, xm, in_sem.at[8])
    factor_load = pltpu.make_async_copy(factor_hbm, factor, in_sem.at[13])
    y_loads = [
        pltpu.make_async_copy(ym_hbm.at[pl.ds(pl.multiple_of(h * 128, 128), 128), :], ym.at[pl.ds(128 * place, 128), :], in_sem.at[sem])
        for place, h, sem in ((0, other, 9), (1, col, 12))
    ]
    z_load = pltpu.make_async_copy(zm_hbm, zm, in_sem.at[10])
    g_load = pltpu.make_async_copy(g_hbm, g_buf, in_sem.at[11])
    load_u(0, 0).start()
    load_u(0, 1).start()
    x_load.start()
    factor_load.start()
    for f in range(1, FIELDS):
        load_u(f, 0).start()
        load_u(f, 1).start()
    for load in y_loads:
        load.start()
    z_load.start()
    g_load.start()
    x_load.wait()
    factor_load.wait()

    def x_step(f, half):
        for k in range(2):
            low, high = [
                [u_buf[f, part, pl.ds(first + 2 * half + k, 128, stride=4), :] for part in range(2)]
                for first in (0, 512)
            ]
            for parity, pair in enumerate(even_odd(low, high, factor[0], factor[1])):
                for part in range(2):
                    cols[half, pl.ds(part * 128, 128), pl.ds((2 * k + parity) * 128, 128)] = pair[part]
        out = jnp.dot(xm[...], cols[half], precision=HIGHEST, preferred_element_type=F32)
        for k in range(2):
            rows = send.at[f, 2 * half + k].reshape(512, 128)
            for parity in range(2):
                rows[pl.ds(parity, 256, stride=2), :] = out[:, (2 * k + parity) * 128 : (2 * k + parity) * 128 + 128]

    bufs = (send, hop1, hop2, recv)

    def line(ref, f, yy, dim, at):
        where = [slice(None)] * 3
        where[dim] = at
        return ref.at[(f, yy, *where)]

    def arrived(f, phase, yy):
        three = bufs[phase + 1].at[f, yy, pl.ds(0, 3)]
        pltpu.make_async_copy(three, three, recv_sem.at[phase, f, yy]).wait()

    def forward(f, phase, blocks=range(4)):
        cur, nxt = bufs[phase], bufs[phase + 1]

        def unit(yy, stream):
            dim = STREAMS[stream][phase]
            if phase:
                arrived(f, phase - 1, yy)
            for step in (2, 1, 3):
                there, to = mate(dim, step)
                pltpu.make_async_remote_copy(
                    src_ref=line(cur, f, yy, dim, there),
                    dst_ref=line(nxt, f, yy, dim, coord[dim]),
                    send_sem=send_sem.at[phase, f, yy],
                    recv_sem=recv_sem.at[phase, f, yy],
                    device_id=(0, col, to),
                    device_id_type=MESH,
                ).start()
            line(nxt, f, yy, dim, coord[dim])[...] = line(cur, f, yy, dim, coord[dim])[...]

        for yy in blocks:
            if yy < 3:
                unit(yy, yy)
        for stream in range(3 if 3 in blocks else 0):

            @pl.when(f % 3 == stream)
            def _():
                unit(3, stream)

    def pair_copy(f, p):
        return pltpu.make_async_remote_copy(
            src_ref=ysend.at[f, p],
            dst_ref=zbuf.at[f, p, col],
            send_sem=pair_send.at[2 * f + p],
            recv_sem=pair_recv.at[2 * f + p],
            device_id=(0, other, row),
            device_id_type=MESH,
        )

    def y_step(f):
        for p in range(2):
            for yy in range(4):
                rows = recv.at[f, yy].reshape(512, 128)
                turn = pl.ds(yy * 32, 32)
                for k in range(2):
                    low, high = [
                        [rows[pl.ds(first + part * 4 + 2 * p + k, 32, stride=8), :] for part in range(2)]
                        for first in (0, 256)
                    ]
                    for parity, pair in enumerate(even_odd(low, high, factor[2, turn, :], factor[3, turn, :])):
                        for part in range(2):
                            planes[p, pl.ds(part * 128 + yy * 32, 32), pl.ds((2 * k + parity) * 128, 128)] = pair[part]
            out = jnp.dot(ym[...], planes[p], precision=HIGHEST, preferred_element_type=F32)
            for part in range(2):
                for k in range(2):
                    for parity in range(2):
                        lanes = slice((2 * k + parity) * 128, (2 * k + parity) * 128 + 128)
                        where = pl.ds(k * 128 + parity, 64, stride=2)
                        ysend[f, p, part, where, :] = out[part * 64 : part * 64 + 64, lanes]
                        zbuf[f, p, col, part, where, :] = out[128 + part * 64 : 128 + part * 64 + 64, lanes]
        for p in range(2):
            pair_copy(f, p).start()

    def z_step(f):
        for p in range(2):
            pair_copy(f, p).wait_recv()
        for p in range(2):
            for (part, k), value in z_product(zbuf, zm, g_buf, f, p).items():
                wbuf[f, part, 2 * p + k] = value

    @pl.loop(0, FIELDS + 6)
    def _(t):
        @pl.when(t < FIELDS)
        def _():
            load_u(t, 0).wait()
            load_u(t, 1).wait()
            x_step(t, 0)

            @pl.when(t == 0)
            def _():
                pl.semaphore_wait(barrier, 10)

            forward(t, 0, (0, 1))
            x_step(t, 1)
            forward(t, 0, (2, 3))

        for phase in (1, 2):

            @pl.when((t >= 2 * phase) & (t < FIELDS + 2 * phase))
            def _():
                forward(t - 2 * phase, phase)

        @pl.when(t == 6)
        def _():
            for load in y_loads:
                load.wait()
            z_load.wait()
            g_load.wait()

        @pl.when(t == 7)
        def _():
            z_step(t - 7)

        @pl.when(t >= 6)
        def _():
            for yy in range(4):
                arrived(t - 6, 2, yy)
            y_step(t - 6)

        @pl.when(t >= 8)
        def _():
            z_step(t - 7)

    for p in range(2):
        pair_copy(FIELDS - 1, p).wait_recv()

    @pl.loop(0, FIELDS)
    def _(f):
        for phase in range(3):
            for yy in range(4):
                three = bufs[phase].at[f, yy, pl.ds(0, 3)]
                pltpu.make_async_copy(three, three, send_sem.at[phase, f, yy]).wait()
        for p in range(2):
            pair_copy(f, p).wait_send()


def solution(mesh):
    mats = matrices()

    def local_forward(u_real, u_imag, g_filter):
        flat = (FIELDS, 4 * N, 128)
        hbm_spec = pl.BlockSpec(memory_space=pltpu.HBM)
        vmem_spec = pl.BlockSpec(memory_space=pltpu.VMEM)
        kept = pl.pallas_call(
            kernel,
            out_shape=(
                pltpu.VMEM((FIELDS, 2, 2, 2, 256, 128), F32),
                pltpu.VMEM((FIELDS - 1, 2, 4, 128, N), F32),
                pltpu.VMEM((512, 512), F32),
                pltpu.VMEM((4, 128, N), F32),
            ),
            in_specs=[hbm_spec] * 7,
            out_specs=(vmem_spec,) * 4,
            scratch_shapes=[
                pltpu.VMEM((FIELDS, 2, 4 * N, 128), F32),
                pltpu.VMEM((256, 256), F32),
                pltpu.VMEM((256, 256), F32),
                pltpu.VMEM((4, 128, 128), F32),
                pltpu.VMEM((2, 256, 512), F32),
                *[pltpu.VMEM((FIELDS, 4, 4, 4, 4, 8, 128), F32)] * 4,
                pltpu.VMEM((2, 256, 512), F32),
                pltpu.VMEM((FIELDS, 2, 2, 256, 128), F32),
                pltpu.SemaphoreType.DMA((14,)),
                pltpu.SemaphoreType.DMA((3, FIELDS, 4)),
                pltpu.SemaphoreType.DMA((3, FIELDS, 4)),
                pltpu.SemaphoreType.DMA((2 * FIELDS,)),
                pltpu.SemaphoreType.DMA((2 * FIELDS,)),
            ],
            compiler_params=pltpu.CompilerParams(collective_id=0, has_side_effects=True, vmem_limit_bytes=55 * 2**20),
        )(u_real.reshape(flat), u_imag.reshape(flat), g_filter, *[jnp.asarray(m) for m in mats])
        out = jax.ShapeDtypeStruct((FIELDS, 4, 128, N), F32)
        return pl.pallas_call(
            last_kernel,
            out_shape=(out, out),
            in_specs=[vmem_spec] * 4,
            out_specs=(hbm_spec, hbm_spec),
            scratch_shapes=[
                pltpu.VMEM((2, 4, 128, N), F32),
                pltpu.SemaphoreType.DMA((2 * FIELDS - 2,)),
                pltpu.SemaphoreType.DMA((4,)),
            ],
            compiler_params=pltpu.CompilerParams(vmem_limit_bytes=40 * 2**20),
        )(*kept)

    field_spec = P("fld", None, "row", "col")
    out_spec = P("fld", "row", "col", None)
    return jax.shard_map(local_forward, mesh=mesh, in_specs=(field_spec, field_spec, P("row", "col", None)), out_specs=(out_spec, out_spec), check_vma=False)
```

```python
import jax
import jax.numpy as jnp
import numpy as np
from jax import lax
from jax.experimental import pallas as pl
from jax.experimental.pallas import tpu as pltpu
from jax.sharding import PartitionSpec as P

MESH = pl.DeviceIdType.MESH
N = 256
FIELDS = 4
SCALE = 1.0 / 16.0
HIGHEST = lax.Precision.HIGHEST
F32 = jnp.float32


def dft_blocks(length):
    steps = np.outer(np.arange(length), np.arange(length)) % length
    angles = steps * (2.0 * np.pi / length)
    cos_part, sin_part = np.cos(angles), np.sin(angles)
    real_rows = np.stack([cos_part, sin_part], axis=1)
    imag_rows = np.stack([-sin_part, cos_part], axis=1)
    return np.stack([real_rows, imag_rows])


def matrices():
    half, full = dft_blocks(N // 2), dft_blocks(N) * SCALE
    x_mat = half.reshape(2, 64, 2, 2, 128).transpose(1, 0, 2, 3, 4).reshape(256, 256)
    y_mat = half.reshape(2, 2, 64, 2, 32, 4).transpose(1, 0, 2, 3, 5, 4).reshape(256, 256)
    z_mat = full.transpose(2, 3, 0, 1).reshape(512, 512)
    turns = np.arange(N // 2) * (2.0 * np.pi / N)
    y_turns = turns.reshape(32, 4).T.reshape(-1)
    factors = np.stack([np.cos(turns), np.sin(turns), np.cos(y_turns), np.sin(y_turns)])
    factors = np.repeat(factors[:, :, None], 128, axis=2)
    return [m.astype(np.float32) for m in (x_mat, y_mat, z_mat, factors)]


def even_odd(low, high, cos, sin):
    low, high = [v * SCALE for v in low], [v * SCALE for v in high]
    even = [a + b for a, b in zip(low, high)]
    re, im = [a - b for a, b in zip(low, high)]
    return even, [re * cos + im * sin, im * cos - re * sin]


STREAMS = ((2, 1, 0), (1, 0, 2), (0, 2, 1))


def z_product(zbuf, zm, g_buf, f, p):
    lines = jnp.concatenate([zbuf[f, p, h, part] for part in range(2) for h in range(2)], axis=1)
    out = jnp.dot(lines, zm[...], precision=HIGHEST, preferred_element_type=F32)
    return {
        (part, k): out[k * 128 : k * 128 + 128, part * 256 : part * 256 + 256] * g_buf[2 * p + k]
        for part in range(2)
        for k in range(2)
    }


def last_kernel(zbuf, wbuf, zm, g_buf, wr_hbm, wi_hbm, w_last, out_sem, last_sem):
    outs = (wr_hbm, wi_hbm)
    done = [
        pltpu.make_async_copy(wbuf.at[f, part], outs[part].at[f], out_sem.at[2 * f + part])
        for f in range(FIELDS - 1)
        for part in range(2)
    ]
    for copy in done:
        copy.start()
    last = FIELDS - 1
    for p in range(2):
        for (part, k), value in z_product(zbuf, zm, g_buf, last, p).items():
            w_last[part, 2 * p + k] = value
        for part in range(2):
            copy = pltpu.make_async_copy(w_last.at[part, pl.ds(2 * p, 2)], outs[part].at[last, pl.ds(2 * p, 2)], last_sem.at[2 * p + part])
            copy.start()
            done.append(copy)
    for copy in done:
        copy.wait()


def kernel(ur_hbm, ui_hbm, g_hbm, xm_hbm, ym_hbm, zm_hbm, factor_hbm, zbuf, wbuf, zm, g_buf,
           u_buf, xm, ym, factor, cols, send, hop1, hop2, recv, planes, ysend,
           in_sem, send_sem, recv_sem, pair_send, pair_recv):
    row, col = lax.axis_index("row"), lax.axis_index("col")
    other = 1 - col
    coord = (row // 16, (row // 4) % 4, row % 4)
    stride = (16, 4, 1)

    def mate(dim, step):
        there = (coord[dim] + step) % 4
        return there, row + (there - coord[dim]) * stride[dim]

    barrier = pltpu.get_barrier_semaphore()
    pl.semaphore_signal(barrier, 1, device_id=(0, other, row), device_id_type=MESH)
    for step in (1, 3, 2):
        for dim in range(3):
            pl.semaphore_signal(barrier, 1, device_id=(0, col, mate(dim, step)[1]), device_id_type=MESH)

    def load_u(f, part):
        src = (ur_hbm, ui_hbm)[part]
        return pltpu.make_async_copy(src.at[f], u_buf.at[f, part], in_sem.at[2 * f + part])

    x_load = pltpu.make_async_copy(xm_hbm, xm, in_sem.at[8])
    factor_load = pltpu.make_async_copy(factor_hbm, factor, in_sem.at[13])
    y_loads = [
        pltpu.make_async_copy(ym_hbm.at[pl.ds(pl.multiple_of(h * 128, 128), 128), :], ym.at[pl.ds(128 * place, 128), :], in_sem.at[sem])
        for place, h, sem in ((0, other, 9), (1, col, 12))
    ]
    z_load = pltpu.make_async_copy(zm_hbm, zm, in_sem.at[10])
    g_load = pltpu.make_async_copy(g_hbm, g_buf, in_sem.at[11])
    load_u(0, 0).start()
    load_u(0, 1).start()
    x_load.start()
    factor_load.start()
    for f in range(1, FIELDS):
        load_u(f, 0).start()
        load_u(f, 1).start()
    for load in y_loads:
        load.start()
    z_load.start()
    g_load.start()
    x_load.wait()
    factor_load.wait()

    def x_step(f, half):
        for k in range(2):
            low, high = [
                [u_buf[f, part, pl.ds(first + 2 * half + k, 128, stride=4), :] for part in range(2)]
                for first in (0, 512)
            ]
            for parity, pair in enumerate(even_odd(low, high, factor[0], factor[1])):
                for part in range(2):
                    cols[half, pl.ds(part * 128, 128), pl.ds((2 * k + parity) * 128, 128)] = pair[part]
        out = jnp.dot(xm[...], cols[half], precision=HIGHEST, preferred_element_type=F32)
        for k in range(2):
            rows = send.at[f, 2 * half + k].reshape(512, 128)
            for parity in range(2):
                rows[pl.ds(parity, 256, stride=2), :] = out[:, (2 * k + parity) * 128 : (2 * k + parity) * 128 + 128]

    bufs = (send, hop1, hop2, recv)

    def line(ref, f, yy, dim, at):
        where = [slice(None)] * 3
        where[dim] = at
        return ref.at[(f, yy, *where)]

    def arrived(f, phase, yy):
        three = bufs[phase + 1].at[f, yy, pl.ds(0, 3)]
        pltpu.make_async_copy(three, three, recv_sem.at[phase, f, yy]).wait()

    def forward(f, phase, blocks=range(4)):
        cur, nxt = bufs[phase], bufs[phase + 1]

        def unit(yy, stream):
            dim = STREAMS[stream][phase]
            if phase:
                arrived(f, phase - 1, yy)
            for step in (2, 1, 3):
                there, to = mate(dim, step)
                pltpu.make_async_remote_copy(
                    src_ref=line(cur, f, yy, dim, there),
                    dst_ref=line(nxt, f, yy, dim, coord[dim]),
                    send_sem=send_sem.at[phase, f, yy],
                    recv_sem=recv_sem.at[phase, f, yy],
                    device_id=(0, col, to),
                    device_id_type=MESH,
                ).start()
            line(nxt, f, yy, dim, coord[dim])[...] = line(cur, f, yy, dim, coord[dim])[...]

        for yy in blocks:
            if yy < 3:
                unit(yy, yy)
        for stream in range(3 if 3 in blocks else 0):

            @pl.when((f + 2) % 3 == stream)
            def _():
                unit(3, stream)

    def pair_copy(f, p):
        return pltpu.make_async_remote_copy(
            src_ref=ysend.at[f, p],
            dst_ref=zbuf.at[f, p, col],
            send_sem=pair_send.at[2 * f + p],
            recv_sem=pair_recv.at[2 * f + p],
            device_id=(0, other, row),
            device_id_type=MESH,
        )

    def y_step(f):
        for p in range(2):
            for yy in range(4):
                rows = recv.at[f, yy].reshape(512, 128)
                turn = pl.ds(yy * 32, 32)
                for k in range(2):
                    low, high = [
                        [rows[pl.ds(first + part * 4 + 2 * p + k, 32, stride=8), :] for part in range(2)]
                        for first in (0, 256)
                    ]
                    for parity, pair in enumerate(even_odd(low, high, factor[2, turn, :], factor[3, turn, :])):
                        for part in range(2):
                            planes[p, pl.ds(part * 128 + yy * 32, 32), pl.ds((2 * k + parity) * 128, 128)] = pair[part]
            out = jnp.dot(ym[...], planes[p], precision=HIGHEST, preferred_element_type=F32)
            for part in range(2):
                for k in range(2):
                    for parity in range(2):
                        lanes = slice((2 * k + parity) * 128, (2 * k + parity) * 128 + 128)
                        where = pl.ds(k * 128 + parity, 64, stride=2)
                        ysend[f, p, part, where, :] = out[part * 64 : part * 64 + 64, lanes]
                        zbuf[f, p, col, part, where, :] = out[128 + part * 64 : 128 + part * 64 + 64, lanes]
        for p in range(2):
            pair_copy(f, p).start()

    def z_step(f):
        for p in range(2):
            pair_copy(f, p).wait_recv()
        for p in range(2):
            for (part, k), value in z_product(zbuf, zm, g_buf, f, p).items():
                wbuf[f, part, 2 * p + k] = value

    @pl.loop(0, FIELDS + 6)
    def _(t):
        @pl.when(t < FIELDS)
        def _():
            load_u(t, 0).wait()
            load_u(t, 1).wait()
            x_step(t, 0)

            @pl.when(t == 0)
            def _():
                pl.semaphore_wait(barrier, 10)

            forward(t, 0, (0, 1))
            x_step(t, 1)
            forward(t, 0, (2, 3))

        for phase in (1, 2):

            @pl.when((t >= 2 * phase) & (t < FIELDS + 2 * phase))
            def _():
                forward(t - 2 * phase, phase)

        @pl.when(t == 6)
        def _():
            for load in y_loads:
                load.wait()
            z_load.wait()
            g_load.wait()

        @pl.when(t == 7)
        def _():
            z_step(t - 7)

        @pl.when(t >= 6)
        def _():
            for yy in range(4):
                arrived(t - 6, 2, yy)
            y_step(t - 6)

        @pl.when(t >= 8)
        def _():
            z_step(t - 7)

    for p in range(2):
        pair_copy(FIELDS - 1, p).wait_recv()

    @pl.loop(0, FIELDS)
    def _(f):
        for phase in range(3):
            for yy in range(4):
                three = bufs[phase].at[f, yy, pl.ds(0, 3)]
                pltpu.make_async_copy(three, three, send_sem.at[phase, f, yy]).wait()
        for p in range(2):
            pair_copy(f, p).wait_send()


def solution(mesh):
    mats = matrices()

    def local_forward(u_real, u_imag, g_filter):
        flat = (FIELDS, 4 * N, 128)
        hbm_spec = pl.BlockSpec(memory_space=pltpu.HBM)
        vmem_spec = pl.BlockSpec(memory_space=pltpu.VMEM)
        kept = pl.pallas_call(
            kernel,
            out_shape=(
                pltpu.VMEM((FIELDS, 2, 2, 2, 256, 128), F32),
                pltpu.VMEM((FIELDS - 1, 2, 4, 128, N), F32),
                pltpu.VMEM((512, 512), F32),
                pltpu.VMEM((4, 128, N), F32),
            ),
            in_specs=[hbm_spec] * 7,
            out_specs=(vmem_spec,) * 4,
            scratch_shapes=[
                pltpu.VMEM((FIELDS, 2, 4 * N, 128), F32),
                pltpu.VMEM((256, 256), F32),
                pltpu.VMEM((256, 256), F32),
                pltpu.VMEM((4, 128, 128), F32),
                pltpu.VMEM((2, 256, 512), F32),
                *[pltpu.VMEM((FIELDS, 4, 4, 4, 4, 8, 128), F32)] * 4,
                pltpu.VMEM((2, 256, 512), F32),
                pltpu.VMEM((FIELDS, 2, 2, 256, 128), F32),
                pltpu.SemaphoreType.DMA((14,)),
                pltpu.SemaphoreType.DMA((3, FIELDS, 4)),
                pltpu.SemaphoreType.DMA((3, FIELDS, 4)),
                pltpu.SemaphoreType.DMA((2 * FIELDS,)),
                pltpu.SemaphoreType.DMA((2 * FIELDS,)),
            ],
            compiler_params=pltpu.CompilerParams(collective_id=0, has_side_effects=True, vmem_limit_bytes=55 * 2**20),
        )(u_real.reshape(flat), u_imag.reshape(flat), g_filter, *[jnp.asarray(m) for m in mats])
        out = jax.ShapeDtypeStruct((FIELDS, 4, 128, N), F32)
        return pl.pallas_call(
            last_kernel,
            out_shape=(out, out),
            in_specs=[vmem_spec] * 4,
            out_specs=(hbm_spec, hbm_spec),
            scratch_shapes=[
                pltpu.VMEM((2, 4, 128, N), F32),
                pltpu.SemaphoreType.DMA((2 * FIELDS - 2,)),
                pltpu.SemaphoreType.DMA((4,)),
            ],
            compiler_params=pltpu.CompilerParams(vmem_limit_bytes=40 * 2**20),
        )(*kept)

    field_spec = P("fld", None, "row", "col")
    out_spec = P("fld", "row", "col", None)
    return jax.shard_map(local_forward, mesh=mesh, in_specs=(field_spec, field_spec, P("row", "col", None)), out_specs=(out_spec, out_spec), check_vma=False)
```
